32 devices in a mesh: dp: 1, tp: 32 (over x, y, z, core).
Axes of the slice: x: 2, y: 2, z: 4, core: 2. Of those that a mesh axis runs over, the one named last changes fastest.
Arguments:
- x: bfloat16 [2048, 1024], P('dp')
- gain: bfloat16 [1024], replicated
- wq: bfloat16 [1024, 16384], P(None, 'tp')
- wk: bfloat16 [1024, 16384], P(None, 'tp')
- wv: bfloat16 [1024, 16384], P(None, 'tp')
- wo: bfloat16 [16384, 1024], P('tp')
Outputs:
- output: bfloat16 [2048, 1024], P('dp')
All inputs are finite; a program needn't handle non-finite values.
Results may differ from the reference program's by a relative error of at most 0.012.
Values are sent between devices in bfloat16 or wider.
A program may use at most 2 GiB of HBM per device.

```python
import jax
import jax.numpy as jnp
from jax import lax

ROWS = 2048
D = 1024
HEADS = 128
KV_HEADS = 128
HEAD = 128
THETA = 10000


def setup_inputs(seed: int = 0, part: int = 0) -> dict:
    kx, kn, kq, kk, kv, ko = jax.random.split(jax.random.key(seed), 6)

    def weights(key, rows, columns):
        return jax.random.normal(key, (rows, columns), jnp.float32) * rows**-0.5

    drawn = {
        "x": jax.random.normal(jax.random.fold_in(kx, part), (ROWS, D), jnp.float32),
        "gain": 1 + 0.1 * jax.random.normal(kn, (D,), jnp.float32),
        "wq": 2 * weights(kq, D, HEADS * HEAD),
        "wk": 2 * weights(kk, D, KV_HEADS * HEAD),
        "wv": 4 * weights(kv, D, KV_HEADS * HEAD),
        "wo": weights(ko, HEADS * HEAD, D),
    }
    return {k: v.astype(jnp.bfloat16) for k, v in drawn.items()}


def normed(x, gain):
    wide = x.astype(jnp.float32)
    scale = lax.rsqrt(jnp.mean(wide * wide, -1, keepdims=True) + 1e-6)
    return (wide * scale * gain.astype(jnp.float32)).astype(jnp.bfloat16)


def turned(t, place, theta):
    half = t.shape[-1] // 2
    angle = place.astype(jnp.float32)[:, None] * theta ** (-jnp.arange(half, dtype=jnp.float32) / half)
    cos, sin = jnp.cos(angle)[:, None], jnp.sin(angle)[:, None]
    a, b = t[..., :half].astype(jnp.float32), t[..., half:].astype(jnp.float32)
    return jnp.concatenate([a * cos - b * sin, b * cos + a * sin], -1).astype(jnp.bfloat16)


def matmul(a, w):
    return jnp.dot(a, w, preferred_element_type=jnp.float32).astype(jnp.bfloat16)


def einsum(form, a, b):
    return jnp.einsum(form, a.astype(jnp.float32), b.astype(jnp.float32))


def attention(q, k, v):
    scores = einsum("tgsd,ugd->gstu", q, k) * q.shape[-1] ** -0.5
    token = jnp.arange(q.shape[0])
    scores = jnp.where(token[:, None] >= token, scores, -jnp.inf)
    weights = jax.nn.softmax(scores, -1).astype(jnp.bfloat16)
    return einsum("gstu,ugd->tgsd", weights, v).astype(jnp.bfloat16)


def reference(x, gain, wq, wk, wv, wo):
    a, place = normed(x, gain), jnp.arange(ROWS)
    q = turned(matmul(a, wq).reshape(ROWS, HEADS, HEAD), place, THETA).reshape(ROWS, KV_HEADS, -1, HEAD)
    k = turned(matmul(a, wk).reshape(ROWS, KV_HEADS, HEAD), place, THETA)
    v = matmul(a, wv).reshape(ROWS, KV_HEADS, HEAD)
    seen = attention(q, k, v).reshape(ROWS, HEADS * HEAD)
    return (x.astype(jnp.float32) + jnp.dot(seen, wo, preferred_element_type=jnp.float32)).astype(jnp.bfloat16)
```

```python
import functools

import jax
import jax.numpy as jnp
import numpy as np
from jax import lax
from jax.experimental import pallas as pl
from jax.experimental.pallas import tpu as pltpu
from jax.sharding import PartitionSpec as P

HEAD = 128
THETA = 10000
LOG2E = 1.4426950408889634
HIDDEN = -2e30
CH = 256
MESH = pl.DeviceIdType.MESH


def tables():
    half = HEAD // 2
    freq = THETA ** (-np.arange(half, dtype=np.float64) / half)
    freq = np.concatenate([freq, freq])
    sign = np.concatenate([-np.ones(half), np.ones(half)])

    def pair(place):
        angle = place[:, None] * freq
        return np.stack([np.cos(angle), np.sin(angle) * sign]).astype(np.float32)

    return pair(np.arange(8) * CH), pair(np.arange(CH))


def dot(a, b, ca, cb):
    return lax.dot_general(a, b, (((ca,), (cb,)), ((), ())), preferred_element_type=jnp.float32)


def kernel(compute_on, comm_on, x_hbm, gain_ref, wq_hbm, wk_hbm, wv_hbm, wo_hbm, base_ref, local_ref, y_out,
           xs, wq, wk, wv, wo, wvt, ks, vts, qs, seen_s, s_s, top_s, acc_s, sum_s,
           send0, recv0, keep0, send1, recv1, keep1, send2, recv2, keep2, send3, recv3, keep3, y_s,
           load_sem, out_sem, send_sem, recv_sem):
    f32, bf16 = jnp.float32, jnp.bfloat16
    rows, width = xs.shape
    n = rows // CH
    heads = ks.shape[1] // HEAD
    half, quarter = CH // 2, CH // 4
    eighth = CH // 8
    cols = width // 4

    me = lax.axis_index("tp")
    c, z, by, bx = lax.rem(me, 2), lax.rem(me // 2, 4), lax.rem(me // 8, 2), me // 16
    b1 = bx * (1 - c) + by * c
    b2 = by * (1 - c) + bx * c
    p0 = me + 1 - 2 * c
    p1 = me + (16 * (1 - c) + 8 * c) * (1 - 2 * b1)
    p2 = me + (8 * (1 - c) + 16 * c) * (1 - 2 * b2)
    zs = [lax.rem(z + d, 4) for d in (1, 2, 3)]
    pz = [me + 2 * (to - z) for to in zs]

    barrier = pltpu.get_barrier_semaphore()
    for other in (p0, p1, p2, *pz):
        pl.semaphore_signal(barrier, inc=1, device_id={"tp": other}, device_id_type=MESH)

    loads = [pltpu.make_async_copy(a, b, load_sem.at[i]) for i, (a, b) in enumerate(((wq_hbm, wq), (wk_hbm, wk), (wv_hbm, wv), (wo_hbm, wo)))]

    def rows_in(i):
        at = pl.ds(pl.multiple_of(i * CH, CH), CH)
        return pltpu.make_async_copy(x_hbm.at[at], xs.at[at], load_sem.at[4 + i])

    rows_in(0).start()
    for copy in loads:
        copy.start()
    for i in range(1, n):
        rows_in(i).start()
    ks[...] = jnp.zeros(ks.shape, bf16)
    vts[...] = jnp.zeros(vts.shape, bf16)
    for copy in loads:
        copy.wait()
    wvt[...] = wv[...].T
    pl.semaphore_wait(barrier, 6)

    e = HEAD**-0.5 * LOG2E

    def compute(i):
        rows_in(i).wait()
        here = pl.ds(pl.multiple_of(i * CH, CH), CH)
        wide = xs[here, :].astype(f32)
        scale = lax.rsqrt(jnp.mean(wide * wide, -1, keepdims=True) + 1e-6)
        a = (wide * scale * gain_ref[...].astype(f32)).astype(bf16)
        cb, sb = local_ref[0], local_ref[1]
        ca, sa = base_ref[0, pl.ds(i, 1), :], base_ref[1, pl.ds(i, 1), :]
        cos, sin = ca * cb - sa * sb, sa * cb + ca * sb

        def turned(t):
            t = t.astype(bf16).astype(f32)
            return jnp.concatenate(
                [t[:, h * HEAD : (h + 1) * HEAD] * cos + pltpu.roll(t[:, h * HEAD : (h + 1) * HEAD], HEAD // 2, 1) * sin for h in range(heads)], 1
            ).astype(bf16)

        qs[...] = turned(dot(a, wq[...], 1, 0))
        ks[here, :] = turned(dot(a, wk[...], 1, 0))
        vts[:, here] = dot(wvt[...], a, 1, 1).astype(bf16)

        last = i // 2

        def scores(j, tops, masked):
            at = pl.ds(pl.multiple_of(j * 2 * CH, 2 * CH), 2 * CH)
            got = []
            for h in range(heads):
                s = dot(ks[at, h * HEAD : (h + 1) * HEAD], qs[:, h * HEAD : (h + 1) * HEAD], 1, 1)
                if masked:
                    gap = lax.broadcasted_iota(jnp.int32, s.shape, 1) - lax.broadcasted_iota(jnp.int32, s.shape, 0)
                    s = jnp.where(gap >= j * 2 * CH - i * CH, s, HIDDEN)
                s_s[h, j] = s
                got.append(jnp.maximum(tops[h], s.reshape(-1, 8, CH).max(0)))
            return tuple(got)

        tops = scores(last, (jnp.full((8, CH), HIDDEN, f32),) * heads, True)
        tops = lax.fori_loop(0, last, lambda j, t: scores(j, t, False), tops)
        tops = [t.max(0, keepdims=True) for t in tops]

        def weigh(j, sums, first):
            at = pl.ds(pl.multiple_of(j * 2 * CH, 2 * CH), 2 * CH)
            got = []
            for h in range(heads):
                p = jnp.exp2((s_s[h, j] - tops[h]) * e)
                got.append(sums[h] + p.reshape(-1, 8, CH).sum(0))
                o = dot(vts[h * HEAD : (h + 1) * HEAD, at], p.astype(bf16), 1, 0)
                acc_s[h] = o if first else acc_s[h] + o
            return tuple(got)

        sums = weigh(last, (jnp.zeros((8, CH), f32),) * heads, True)
        sums = lax.fori_loop(0, last, lambda j, t: weigh(j, t, False), sums)
        for h in range(heads):
            o = acc_s[h] * (1 / sums[h].sum(0, keepdims=True))
            seen_s[:, h * HEAD : (h + 1) * HEAD] = o.astype(bf16).T

        seen = seen_s[...]
        mine = pl.ds(pl.multiple_of(c * half, half), half)
        theirs = pl.ds(pl.multiple_of((1 - c) * half, half), half)
        send0[i] = dot(seen_s[theirs, :], wo[...], 1, 0).astype(bf16)
        keep0[i] = dot(seen_s[mine, :], wo[...], 1, 0)

    def copy(i, slot, src, dst, to):
        return pltpu.make_async_remote_copy(
            src_ref=src, dst_ref=dst, send_sem=send_sem.at[i, slot], recv_sem=recv_sem.at[i, slot],
            device_id={"tp": to}, device_id_type=MESH)

    def place(i, level):
        at = i * CH
        if level > 0:
            at += c * half
        if level > 1:
            at += b1 * quarter
        if level > 2:
            at += b2 * eighth
        return pl.ds(pl.multiple_of(at, eighth), (CH, half, quarter, eighth)[level])

    def pieces(i):
        return y_s.at[place(i, 3), pl.ds(pl.multiple_of(z * cols, cols), cols)]

    def copies(i, stage):
        if stage == 0:
            return [copy(i, 0, send0.at[i], recv0.at[i], p0)]
        if stage == 1:
            return [copy(i, 1, send1.at[i], recv1.at[i], p1)]
        if stage == 2:
            return [copy(i, 2, send2.at[i], recv2.at[i], p2)]
        if stage == 3:
            return [copy(i, 3 + d, send3.at[i, d], recv3.at[i, d], pz[d]) for d in range(3)]
        if stage == 4:
            return [copy(i, 6 + d, pieces(i), pieces(i), pz[d]) for d in range(3)]
        if stage == 5:
            return [copy(i, 9, y_s.at[place(i, 3)], y_s.at[place(i, 3)], p2)]
        if stage == 6:
            return [copy(i, 10, y_s.at[place(i, 2)], y_s.at[place(i, 2)], p1)]
        return [copy(i, 11, y_s.at[place(i, 1)], y_s.at[place(i, 1)], p0)]

    def start(i, stage):
        for one in copies(i, stage):
            one.start()

    def arrive(i, stage):
        for one in copies(i, stage):
            one.wait()

    def out(i):
        at = pl.ds(pl.multiple_of(i * CH, CH), CH)
        return pltpu.make_async_copy(y_s.at[at], y_out.at[at], out_sem.at[i])

    def step(i, stage):
        arrive(i, stage - 1)
        if stage == 1:
            for b, k in ((b1, True), (1 - b1, False)):
                at = pl.ds(pl.multiple_of(b * quarter, quarter), quarter)
                total = keep0[i, at, :] + recv0[i, at, :].astype(f32)
                if k:
                    keep1[i] = total
                else:
                    send1[i] = total.astype(bf16)
        if stage == 2:
            for b, k in ((b2, True), (1 - b2, False)):
                at = pl.ds(pl.multiple_of(b * eighth, eighth), eighth)
                total = keep1[i, at, :] + recv1[i, at, :].astype(f32)
                if k:
                    keep2[i] = total
                else:
                    send2[i] = total.astype(bf16)
        if stage == 3:
            for d, to in enumerate([*zs, z]):
                at = pl.ds(pl.multiple_of(to * cols, cols), cols)
                total = keep2[i, :, at] + recv2[i, :, at].astype(f32)
                if d == 3:
                    keep3[i] = total
                else:
                    send3[i, d] = total.astype(bf16)
        if stage == 4:
            total = keep3[i]
            for d in range(3):
                total += recv3[i, d].astype(f32)
            at = pl.ds(pl.multiple_of(z * cols, cols), cols)
            y_s[place(i, 3), at] = (total + xs[place(i, 3), at].astype(f32)).astype(bf16)
        if stage < 8:
            start(i, stage)
        else:
            out(i).start()

    def iteration(t, _):
        if compute_on:
            @pl.when(t < n)
            def _():
                compute(t)
        if comm_on:
            @pl.when(t < n)
            def _():
                start(t, 0)
            for stage in range(1, 9):
                @pl.when((t >= stage) & (t < n + stage))
                def _():
                    step(t - stage, stage)
        return _

    lax.fori_loop(0, n + 8 if comm_on else n, iteration, None)
    for i in range(n):
        if not compute_on:
            rows_in(i).wait()
        if not comm_on:
            out(i).start()
        out(i).wait()


def solution(mesh, compute_on=True, comm_on=True):
    def step(x, gain, wq, wk, wv, wo):
        rows, width = x.shape
        inner = wq.shape[1]
        heads, n = inner // HEAD, rows // CH
        base, local = tables()
        f32, bf16 = jnp.float32, jnp.bfloat16
        vmem, anywhere = pl.BlockSpec(memory_space=pltpu.VMEM), pl.BlockSpec(memory_space=pl.ANY)
        V = pltpu.VMEM
        return pl.pallas_call(
            functools.partial(kernel, compute_on, comm_on),
            out_shape=jax.ShapeDtypeStruct((rows, width), bf16),
            in_specs=[anywhere, vmem, anywhere, anywhere, anywhere, anywhere, vmem, vmem],
            out_specs=anywhere,
            scratch_shapes=[
                V((rows, width), bf16),
                *[V((width, inner), bf16)] * 3, V((inner, width), bf16), V((inner, width), bf16),
                V((rows, inner), bf16), V((inner, rows), bf16), V((CH, inner), bf16), V((CH, inner), bf16),
                V((heads, n // 2, 2 * CH, CH), f32), V((8, CH), f32), V((heads, HEAD, CH), f32), V((8, CH), f32),
                V((n, CH // 2, width), bf16), V((n, CH // 2, width), bf16), V((n, CH // 2, width), f32),
                V((n, CH // 4, width), bf16), V((n, CH // 4, width), bf16), V((n, CH // 4, width), f32),
                V((n, CH // 8, width), bf16), V((n, CH // 8, width), bf16), V((n, CH // 8, width), f32),
                V((n, 3, CH // 8, width // 4), bf16), V((n, 3, CH // 8, width // 4), bf16), V((n, CH // 8, width // 4), f32),
                V((rows, width), bf16),
                pltpu.SemaphoreType.DMA((4 + n,)),
                pltpu.SemaphoreType.DMA((n,)),
                pltpu.SemaphoreType.DMA((n, 12)),
                pltpu.SemaphoreType.DMA((n, 12)),
            ],
            compiler_params=pltpu.CompilerParams(collective_id=0, has_side_effects=True, vmem_limit_bytes=60 * 2**20),
            name="layer",
        )(x, gain.reshape(1, -1), wq, wk, wv, wo, jnp.asarray(base), jnp.asarray(local))

    tokens, columns = P("dp", None), P(None, "tp")
    return jax.shard_map(
        step,
        mesh=mesh,
        in_specs=(tokens, P(None), columns, columns, columns, P("tp", None)),
        out_specs=tokens,
        check_vma=False,
    )
```

```python
import functools

import jax
import jax.numpy as jnp
import numpy as np
from jax import lax
from jax.experimental import pallas as pl
from jax.experimental.pallas import tpu as pltpu
from jax.sharding import PartitionSpec as P

HEAD = 128
THETA = 10000
LOG2E = 1.4426950408889634
HIDDEN = -2e30
CH = 256
SLOW, FAST = 7, 1
MESH = pl.DeviceIdType.MESH


def tables():
    half = HEAD // 2
    freq = THETA ** (-np.arange(half, dtype=np.float64) / half)
    freq = np.concatenate([freq, freq])
    sign = np.concatenate([-np.ones(half), np.ones(half)])

    def pair(place):
        angle = place[:, None] * freq
        return np.stack([np.cos(angle), np.sin(angle) * sign]).astype(np.float32)

    return pair(np.arange(8) * CH), pair(np.arange(CH))


def dot(a, b, ca, cb):
    return lax.dot_general(a, b, (((ca,), (cb,)), ((), ())), preferred_element_type=jnp.float32)


def kernel(compute_on, comm_on, x_hbm, gain_hbm, wq_hbm, wk_hbm, wv_hbm, wo_hbm, base_hbm, local_hbm, y_s,
           base_ref, local_ref, gain_ref, xs, wq, wk, wv, wo, wvt, ks, vts, qs, seen_s, s_s, acc_s,
           send0, recv0, keep0, send1, recv1, keep1, send2, recv2, keep2, send3, recv3, keep3,
           load_sem, send_sem, recv_sem):
    f32, bf16 = jnp.float32, jnp.bfloat16
    rows, width = xs.shape
    n = rows // CH
    heads = ks.shape[1] // HEAD
    half, quarter = CH // 2, CH // 4
    eighth = CH // 8
    cols = width // 4

    me = lax.axis_index("tp")
    c, z, by, bx = lax.rem(me, 2), lax.rem(me // 2, 4), lax.rem(me // 8, 2), me // 16
    b1 = bx * (1 - c) + by * c
    b2 = by * (1 - c) + bx * c
    p0 = me + 1 - 2 * c
    p1 = me + (16 * (1 - c) + 8 * c) * (1 - 2 * b1)
    p2 = me + (8 * (1 - c) + 16 * c) * (1 - 2 * b2)
    zs = [lax.rem(z + d, 4) for d in (1, 2, 3)]
    pz = [me + 2 * (to - z) for to in zs]

    barrier = pltpu.get_barrier_semaphore()
    for other in (p0, p1, p2, *pz):
        pl.semaphore_signal(barrier, inc=1, device_id={"tp": other}, device_id_type=MESH)

    loads = [pltpu.make_async_copy(a, b, load_sem.at[i]) for i, (a, b) in enumerate(
        ((gain_hbm, gain_ref), (wv_hbm, wv), (base_hbm, base_ref), (local_hbm, local_ref), (wq_hbm, wq), (wk_hbm, wk), (wo_hbm, wo)))]

    def rows_in(i):
        at = pl.ds(pl.multiple_of(i * CH, CH), CH)
        return pltpu.make_async_copy(x_hbm.at[at], xs.at[at], load_sem.at[7 + i])

    rows_in(0).start()
    for copy in loads:
        copy.start()
    for i in range(1, n):
        rows_in(i).start()
    ks[...] = jnp.zeros(ks.shape, bf16)
    vts[...] = jnp.zeros(vts.shape, bf16)
    for copy in loads:
        copy.wait()
    wvt[...] = wv[...].T
    e = HEAD**-0.5 * LOG2E

    def compute(i, between):
        rows_in(i).wait()
        here = pl.ds(pl.multiple_of(i * CH, CH), CH)
        wide = xs[here, :].astype(f32)
        scale = lax.rsqrt(jnp.mean(wide * wide, -1, keepdims=True) + 1e-6)
        a = (wide * scale * gain_ref[...].reshape(1, width).astype(f32)).astype(bf16)
        cb, sb = local_ref[0], local_ref[1]
        ca, sa = base_ref[0, pl.ds(i, 1), :], base_ref[1, pl.ds(i, 1), :]
        cos, sin = ca * cb - sa * sb, sa * cb + ca * sb

        def turned(t):
            t = t.astype(bf16).astype(f32)
            return jnp.concatenate(
                [t[:, h * HEAD : (h + 1) * HEAD] * cos + pltpu.roll(t[:, h * HEAD : (h + 1) * HEAD], HEAD // 2, 1) * sin for h in range(heads)], 1
            ).astype(bf16)

        qs[...] = turned(dot(a, wq[...], 1, 0))
        ks[here, :] = turned(dot(a, wk[...], 1, 0))
        vts[:, here] = dot(wvt[...], a, 1, 1).astype(bf16)

        last = i // 2
        ones = jnp.ones((8, 2 * CH), bf16)

        def scores(h, j, masked):
            at = pl.ds(pl.multiple_of(j * 2 * CH, 2 * CH), 2 * CH)
            s = dot(ks[at, h * HEAD : (h + 1) * HEAD], qs[:, h * HEAD : (h + 1) * HEAD], 1, 1) * e
            if masked:
                gap = lax.broadcasted_iota(jnp.int32, s.shape, 1) - lax.broadcasted_iota(jnp.int32, s.shape, 0)
                s = jnp.where(gap >= j * 2 * CH - i * CH, s, HIDDEN)
            s_s[h] = s
            return s.max(0, keepdims=True)

        def weigh(h, j, s, before, top):
            at = pl.ds(pl.multiple_of(j * 2 * CH, 2 * CH), 2 * CH)
            p = jnp.exp2(s - top).astype(bf16)
            values = jnp.concatenate([vts[h * HEAD : (h + 1) * HEAD, at], ones], 0)
            acc_s[h] = acc_s[h] * jnp.exp2(before - top) + dot(values, p, 1, 0)

        for h in range(heads):
            acc_s[h] = jnp.zeros(acc_s.shape[1:], f32)
        tops = tuple(scores(h, last, True) for h in range(heads))

        def trip(j, carry):
            got = []
            for h, (before, top) in enumerate(carry):
                s = s_s[h]
                new = scores(h, j, False)
                weigh(h, jnp.where(j == 0, last, j - 1), s, before, top)
                got.append((top, jnp.maximum(top, new)))
            return tuple(got)

        tops = lax.fori_loop(0, last, trip, tuple((t, t) for t in tops))

        @pl.when(i == 0)
        def _():
            pl.semaphore_wait(barrier, 6)

        if FAST > 1 and SLOW < n - 1:
            between(1)
        for h in range(heads):
            weigh(h, jnp.maximum(last - 1, 0), s_s[h], *tops[h])
            o = acc_s[h, :HEAD] * (1 / acc_s[h, HEAD : HEAD + 1])
            seen_s[:, h * HEAD : (h + 1) * HEAD] = o.astype(bf16).T

        seen = seen_s[...]
        mine = pl.ds(pl.multiple_of(c * half, half), half)
        theirs = pl.ds(pl.multiple_of((1 - c) * half, half), half)
        send0[i] = dot(seen_s[theirs, :], wo[...], 1, 0).astype(bf16)
        keep0[i] = dot(seen_s[mine, :], wo[...], 1, 0)

    def copy(i, slot, src, dst, to):
        return pltpu.make_async_remote_copy(
            src_ref=src, dst_ref=dst, send_sem=send_sem.at[i, slot], recv_sem=recv_sem.at[i, slot],
            device_id={"tp": to}, device_id_type=MESH)

    def place(i, level):
        at = i * CH
        if level > 0:
            at += c * half
        if level > 1:
            at += b1 * quarter
        if level > 2:
            at += b2 * eighth
        return pl.ds(pl.multiple_of(at, eighth), (CH, half, quarter, eighth)[level])

    def pieces(i):
        return y_s.at[place(i, 3), pl.ds(pl.multiple_of(z * cols, cols), cols)]

    def copies(i, stage):
        if stage == 0:
            return [copy(i, 0, send0.at[i], recv0.at[i], p0)]
        if stage == 1:
            return [copy(i, 1, send1.at[i], recv1.at[i], p1)]
        if stage == 2:
            return [copy(i, 2, send2.at[i], recv2.at[i], p2)]
        if stage == 3:
            return [copy(i, 3 + d, send3.at[i, d], recv3.at[i, d], pz[d]) for d in range(3)]
        if stage == 4:
            return [copy(i, 6 + d, pieces(i), pieces(i), pz[d]) for d in range(3)]
        if stage == 5:
            return [copy(i, 9, y_s.at[place(i, 3)], y_s.at[place(i, 3)], p2)]
        if stage == 6:
            return [copy(i, 10, y_s.at[place(i, 2)], y_s.at[place(i, 2)], p1)]
        return [copy(i, 11, y_s.at[place(i, 1)], y_s.at[place(i, 1)], p0)]

    def start(i, stage):
        for one in copies(i, stage):
            one.start()

    def arrive(i, stage):
        for one in copies(i, stage):
            one.wait()

    def step(i, stage):
        arrive(i, stage - 1)
        if stage == 1:
            for b, k in ((b1, True), (1 - b1, False)):
                at = pl.ds(pl.multiple_of(b * quarter, quarter), quarter)
                total = keep0[i, at, :] + recv0[i, at, :].astype(f32)
                if k:
                    keep1[i] = total
                else:
                    send1[i] = total.astype(bf16)
        if stage == 2:
            for b, k in ((b2, True), (1 - b2, False)):
                at = pl.ds(pl.multiple_of(b * eighth, eighth), eighth)
                total = keep1[i, at, :] + recv1[i, at, :].astype(f32)
                if k:
                    keep2[i] = total
                else:
                    send2[i] = total.astype(bf16)
        if stage == 3:
            for d, to in enumerate([*zs, z]):
                at = pl.ds(pl.multiple_of(to * cols, cols), cols)
                total = keep2[i, :, at] + recv2[i, :, at].astype(f32)
                if d == 3:
                    keep3[i] = total
                else:
                    send3[i, d] = total.astype(bf16)
        if stage == 4:
            total = keep3[i]
            for d in range(3):
                total += recv3[i, d].astype(f32)
            at = pl.ds(pl.multiple_of(z * cols, cols), cols)
            y_s[place(i, 3), at] = (total + xs[place(i, 3), at].astype(f32)).astype(bf16)
        if stage < 8:
            start(i, stage)

    def due(i):
        return jnp.minimum(i, SLOW) + FAST * jnp.maximum(i - SLOW, 0)

    def tick(k):
        if comm_on:
            for stage in range(1, 9):
                q = k - stage
                over = jnp.maximum(q - SLOW, 0)
                i = jnp.minimum(q, SLOW) + over // FAST

                @pl.when((q >= 0) & (i < n) & (lax.rem(over, FAST) == 0))
                def _():
                    step(i, stage)

    def iteration(t, _):
        def between(part):
            @pl.when(t > SLOW)
            def _():
                tick(due(t) - FAST + part)

        if compute_on:
            compute(t, between)
        else:
            for part in range(1, FAST):
                between(part)
        if comm_on:
            start(t, 0)
        tick(due(t))
        return _

    if not compute_on:
        pl.semaphore_wait(barrier, 6)
    lax.fori_loop(0, n, iteration, None)
    if comm_on:
        lax.fori_loop(1, 9, lambda k, _: tick(due(n - 1) + k), None)
    if not compute_on:
        for i in range(n):
            rows_in(i).wait()


def solution(mesh, compute_on=True, comm_on=True):
    def step(x, gain, wq, wk, wv, wo):
        rows, width = x.shape
        inner = wq.shape[1]
        heads, n = inner // HEAD, rows // CH
        base, local = tables()
        f32, bf16 = jnp.float32, jnp.bfloat16
        vmem, hbm = pl.BlockSpec(memory_space=pltpu.VMEM), pl.BlockSpec(memory_space=pltpu.HBM)
        V = pltpu.VMEM
        return pl.pallas_call(
            functools.partial(kernel, compute_on, comm_on),
            out_shape=pltpu.VMEM((rows, width), bf16),
            in_specs=[hbm] * 8,
            out_specs=vmem,
            scratch_shapes=[
                V(base.shape, f32), V(local.shape, f32), V((width,), bf16), V((rows, width), bf16),
                *[V((width, inner), bf16)] * 3, V((inner, width), bf16), V((inner, width), bf16),
                V((rows, inner), bf16), V((inner, rows), bf16), V((CH, inner), bf16), V((CH, inner), bf16),
                V((heads, 2 * CH, CH), f32), V((heads, HEAD + 8, CH), f32),
                V((n, CH // 2, width), bf16), V((n, CH // 2, width), bf16), V((n, CH // 2, width), f32),
                V((n, CH // 4, width), bf16), V((n, CH // 4, width), bf16), V((n, CH // 4, width), f32),
                V((n, CH // 8, width), bf16), V((n, CH // 8, width), bf16), V((n, CH // 8, width), f32),
                V((n, 3, CH // 8, width // 4), bf16), V((n, 3, CH // 8, width // 4), bf16), V((n, CH // 8, width // 4), f32),
                pltpu.SemaphoreType.DMA((7 + n,)),
                pltpu.SemaphoreType.DMA((n, 12)),
                pltpu.SemaphoreType.DMA((n, 12)),
            ],
            compiler_params=pltpu.CompilerParams(collective_id=0, has_side_effects=True, vmem_limit_bytes=48 * 2**20),
            name="layer",
        )(x, gain, wq, wk, wv, wo, jnp.asarray(base), jnp.asarray(local))

    tokens, columns = P("dp", None), P(None, "tp")
    return jax.shard_map(
        step,
        mesh=mesh,
        in_specs=(tokens, P(None), columns, columns, columns, P("tp", None)),
        out_specs=tokens,
        check_vma=False,
    )
```

```python
import functools

import jax
import jax.numpy as jnp
import numpy as np
from jax import lax
from jax.experimental import pallas as pl
from jax.experimental.pallas import tpu as pltpu
from jax.sharding import PartitionSpec as P

HEAD = 128
THETA = 10000
LOG2E = 1.4426950408889634
HIDDEN = -2e30
CH = 256
MESH = pl.DeviceIdType.MESH


def tables():
    half = HEAD // 2
    freq = THETA ** (-np.arange(half, dtype=np.float64) / half)
    freq = np.concatenate([freq, freq])
    sign = np.concatenate([-np.ones(half), np.ones(half)])

    def pair(place):
        angle = place[:, None] * freq
        return np.stack([np.cos(angle), np.sin(angle) * sign]).astype(np.float32)

    return pair(np.arange(8) * CH), pair(np.arange(CH))


LONG = ("pair", "first", "second", "line", "line back", "second back", "first back", "pair back")
SHORT = ("pair", "plane", "line", "line back", "plane back", "pair back")
QUICK = 2


def path(i, n):
    return SHORT if i >= n - QUICK else LONG


PLAN = [[], [], [], [0], [], [], [1], [], [0], [], [2], [0, 1], [3], [], [2], [3, 0, 4, 1], [2], [], [5, 3, 4], [1], [0, 2], [5, 4, 3, 6], [], [], [5, 1, 2, 4, 7, 6, 0, 5, 2, 4, 7, 3, 1, 6, 5, 4, 3, 7, 2, 5, 6, 7, 1, 0, 5, 6, 4, 0, 3, 1, 5, 4, 7, 6, 3, 2, 7]]


def layout(n):
    taken = [0] * n
    steps = []
    for chunks in PLAN:
        steps.append([])
        for i in chunks:
            taken[i] += 1
            steps[-1].append((i, taken[i]))
    return {(t, spot): steps[3 * t + spot] for t in range(n) for spot in range(3)}, steps[-1]


def dot(a, b, ca, cb):
    return lax.dot_general(a, b, (((ca,), (cb,)), ((), ())), preferred_element_type=jnp.float32)


def kernel(compute_on, comm_on, x_hbm, gain_hbm, wq_hbm, wk_hbm, wv_hbm, wo_hbm, base_hbm, local_hbm, y_s,
           base_ref, local_ref, gain_ref, xs, wq, wk, wv, wo, wvt, ks, vts, qs, seen_s, s_s, acc_s,
           send0, recv0, keep0, send1, recv1, keep1, send2, recv2, keep2, send3, recv3, keep3,
           load_sem, send_sem, recv_sem):
    f32, bf16 = jnp.float32, jnp.bfloat16
    rows, width = xs.shape
    n = rows // CH
    heads = ks.shape[1] // HEAD
    half, quarter = CH // 2, CH // 4
    eighth, last_rows = CH // 8, CH // 16
    cols = width // 4

    me = lax.axis_index("tp")
    c, z, by, bx = lax.rem(me, 2), lax.rem(me // 2, 4), lax.rem(me // 8, 2), me // 16
    p0 = me + 1 - 2 * c
    px, py = me + 16 * (1 - 2 * bx), me + 8 * (1 - 2 * by)
    b1, b2 = (bx, by), (by, bx)
    p1, p2, p12 = (px, py), (py, px), px + py - me
    zs = [lax.rem(z + d, 4) for d in (1, 2, 3)]
    pz = [me + 2 * (to - z) for to in zs]

    barrier = pltpu.get_barrier_semaphore()
    for other in (p0, px, py, p12, *pz):
        pl.semaphore_signal(barrier, inc=1, device_id={"tp": other}, device_id_type=MESH)

    loads = [pltpu.make_async_copy(a, b, load_sem.at[i]) for i, (a, b) in enumerate(
        ((gain_hbm, gain_ref), (wv_hbm, wv), (base_hbm, base_ref), (local_hbm, local_ref), (wq_hbm, wq), (wk_hbm, wk), (wo_hbm, wo)))]

    def rows_in(i):
        at = pl.ds(pl.multiple_of(i * CH, CH), CH)
        return pltpu.make_async_copy(x_hbm.at[at], xs.at[at], load_sem.at[7 + i])

    rows_in(0).start()
    for copy in loads:
        copy.start()
    for i in range(1, n):
        rows_in(i).start()
    ks[...] = jnp.zeros(ks.shape, bf16)
    vts[...] = jnp.zeros(vts.shape, bf16)
    loads[1].wait()
    wvt[...] = wv[...].T
    for at in (0, 2, 3, 4, 5):
        loads[at].wait()
    e = HEAD**-0.5 * LOG2E

    def compute(i, between):
        rows_in(i).wait()
        here = pl.ds(pl.multiple_of(i * CH, CH), CH)
        wide = xs[here, :].astype(f32)
        scale = lax.rsqrt(jnp.mean(wide * wide, -1, keepdims=True) + 1e-6)
        a = (wide * scale * gain_ref[...].reshape(1, width).astype(f32)).astype(bf16)
        cb, sb = local_ref[0], local_ref[1]
        ca, sa = base_ref[0, pl.ds(i, 1), :], base_ref[1, pl.ds(i, 1), :]
        cos, sin = ca * cb - sa * sb, sa * cb + ca * sb

        def turned(t):
            t = t.astype(bf16).astype(f32)
            return jnp.concatenate(
                [t[:, h * HEAD : (h + 1) * HEAD] * cos + pltpu.roll(t[:, h * HEAD : (h + 1) * HEAD], HEAD // 2, 1) * sin for h in range(heads)], 1
            ).astype(bf16)

        qs[...] = turned(dot(a, wq[...], 1, 0))
        ks[here, :] = turned(dot(a, wk[...], 1, 0))
        vts[:, here] = dot(wvt[...], a, 1, 1).astype(bf16)

        last = i // 2
        ones = jnp.ones((8, 2 * CH), bf16)

        def scores(h, j, masked):
            at = pl.ds(pl.multiple_of(j * 2 * CH, 2 * CH), 2 * CH)
            s = dot(ks[at, h * HEAD : (h + 1) * HEAD], qs[:, h * HEAD : (h + 1) * HEAD], 1, 1) * e
            if masked:
                gap = lax.broadcasted_iota(jnp.int32, s.shape, 1) - lax.broadcasted_iota(jnp.int32, s.shape, 0)
                s = jnp.where(gap >= j * 2 * CH - i * CH, s, HIDDEN)
            s_s[h] = s
            return s.max(0, keepdims=True)

        def weigh(h, j, s, before, top):
            at = pl.ds(pl.multiple_of(j * 2 * CH, 2 * CH), 2 * CH)
            p = jnp.exp2(s - top).astype(bf16)
            values = jnp.concatenate([vts[h * HEAD : (h + 1) * HEAD, at], ones], 0)
            acc_s[h] = acc_s[h] * jnp.exp2(before - top) + dot(values, p, 1, 0)

        for h in range(heads):
            acc_s[h] = jnp.zeros(acc_s.shape[1:], f32)
        tops = tuple(scores(h, last, True) for h in range(heads))

        def trip(j, carry):
            got = []
            for h, (before, top) in enumerate(carry):
                s = s_s[h]
                new = scores(h, j, False)
                weigh(h, jnp.where(j == 0, last, j - 1), s, before, top)
                got.append((top, jnp.maximum(top, new)))
            return tuple(got)

        @pl.when(i == 0)
        def _():
            pl.semaphore_wait(barrier, 7)

        between(0)
        tops = lax.fori_loop(0, last, trip, tuple((t, t) for t in tops))

        between(1)
        for h in range(heads):
            weigh(h, jnp.maximum(last - 1, 0), s_s[h], *tops[h])
            o = acc_s[h, :HEAD] * (1 / acc_s[h, HEAD : HEAD + 1])
            seen_s[:, h * HEAD : (h + 1) * HEAD] = o.astype(bf16).T

        @pl.when(i == 0)
        def _():
            loads[6].wait()

        mine = pl.ds(pl.multiple_of(c * half, half), half)
        theirs = pl.ds(pl.multiple_of((1 - c) * half, half), half)
        send0[i] = dot(seen_s[theirs, :], wo[...], 1, 0).astype(bf16)
        keep0[i] = dot(seen_s[mine, :], wo[...], 1, 0)

    SLOT = {"pair": 0, "first": 1, "plane": 1, "second": 2, "line": 3, "line back": 4, "second back": 5, "plane back": 5, "first back": 6, "pair back": 7}
    ROWS = {"pair": half, "first": quarter, "plane": quarter + eighth, "second": eighth, "line": 3 * eighth // 4, "line back": 3 * eighth // 4,
            "second back": eighth, "plane back": quarter + eighth, "first back": quarter, "pair back": half}

    def copy(i, move, src, dst, to):
        return pltpu.make_async_remote_copy(
            src_ref=src, dst_ref=dst, send_sem=send_sem.at[i], recv_sem=recv_sem.at[i, SLOT[move]],
            device_id={"tp": to}, device_id_type=MESH)

    def place(i, level, o):
        at = i * CH + c * half
        if level > 1:
            at += o * quarter
        if level > 2:
            at += b1[o] * eighth
        if level > 3:
            at += b2[o] * last_rows
        return pl.ds(pl.multiple_of(at, last_rows), (CH, half, quarter, eighth, last_rows)[level])

    def pieces(i, o):
        return y_s.at[place(i, 4, o), pl.ds(pl.multiple_of(z * cols, cols), cols)]

    low, high = pl.ds(0, last_rows), pl.ds(last_rows, last_rows)

    def copies(i, move):
        made = []

        def add(src, dst, to):
            made.append(copy(i, move, src, dst, to))

        if move == "pair":
            add(send0.at[i], recv0.at[i], p0)
        if move == "line":
            for d in range(3):
                add(send3.at[i, d], recv3.at[i, d], pz[d])
        if move == "pair back":
            add(y_s.at[place(i, 1, 0)], y_s.at[place(i, 1, 0)], p0)
        for o in (0, 1):
            own = y_s.at[place(i, 4, o)]
            if move == "first":
                add(send1.at[i, o], recv1.at[i, o], p1[o])
            if move == "second":
                add(send2.at[i, o], recv2.at[i, o], p2[o])
            if move == "plane":
                add(send1.at[i, o, low], recv1.at[i, o, low], p1[o])
                add(send1.at[i, o, high], recv1.at[i, o, high], p2[o])
                add(send2.at[i, o], recv2.at[i, o], p12)
            if move == "line back":
                for d in range(3):
                    add(pieces(i, o), pieces(i, o), pz[d])
            if move == "plane back":
                for to in (p1[o], p2[o], p12):
                    add(own, own, to)
            if move == "second back":
                add(own, own, p2[o])
            if move == "first back":
                add(y_s.at[place(i, 3, o)], y_s.at[place(i, 3, o)], p1[o])
        return made

    def start(i, move):
        for one in copies(i, move):
            one.start()

    def arrive(i, move):
        some = y_s.at[pl.ds(0, ROWS[move])]
        copy(i, move, some, some, p0).wait_recv()

    def gone(i):
        some = y_s.at[pl.ds(0, sum(ROWS[move] for move in LONG))]
        copy(i, "pair", some, some, p0).wait_send()

    def step(i, k):
        moves = path(i, n)
        came, move = moves[k - 1], moves[k] if k < len(moves) else None
        arrive(i, came)
        for o in (0, 1):
            def pair_sum(x1, x2, size):
                at = pl.ds(pl.multiple_of(o * quarter + x1 * eighth + x2 * last_rows, last_rows), size)
                return keep0[i, at, :] + recv0[i, at, :].astype(f32)

            if move == "first":
                keep1[i, o] = pair_sum(b1[o], 0, eighth)
                send1[i, o] = pair_sum(1 - b1[o], 0, eighth).astype(bf16)
            if move == "second":
                for flip in (False, True):
                    at = pl.ds(pl.multiple_of((1 - b2[o] if flip else b2[o]) * last_rows, last_rows), last_rows)
                    total = keep1[i, o, at, :] + recv1[i, o, at, :].astype(f32)
                    if flip:
                        send2[i, o] = total.astype(bf16)
                    else:
                        keep2[i, o] = total
            if move == "plane":
                send1[i, o, low] = pair_sum(1 - b1[o], b2[o], last_rows).astype(bf16)
                send1[i, o, high] = pair_sum(b1[o], 1 - b2[o], last_rows).astype(bf16)
                send2[i, o] = pair_sum(1 - b1[o], 1 - b2[o], last_rows).astype(bf16)
                keep2[i, o] = pair_sum(b1[o], b2[o], last_rows)
            there = (low, high)[o]
            if move == "line":
                for d, to in enumerate([*zs, z]):
                    at = pl.ds(pl.multiple_of(to * cols, cols), cols)
                    total = keep2[i, o, :, at] + recv2[i, o, :, at].astype(f32)
                    if came == "plane":
                        total += recv1[i, o, low, at].astype(f32) + recv1[i, o, high, at].astype(f32)
                    if d == 3:
                        keep3[i, there] = total
                    else:
                        send3[i, d, there] = total.astype(bf16)
            if move == "line back":
                total = keep3[i, there]
                for d in range(3):
                    total += recv3[i, d, there].astype(f32)
                at = pl.ds(pl.multiple_of(z * cols, cols), cols)
                y_s[place(i, 4, o), at] = (total + xs[place(i, 4, o), at].astype(f32)).astype(bf16)
        if move is not None:
            start(i, move)

    sites, drain = layout(n)

    def iteration(t, _):
        def between(spot):
            if comm_on:
                for when in range(n):
                    if sites[when, spot]:
                        @pl.when(t == when)
                        def _():
                            for i, k in sites[when, spot]:
                                step(i, k)

        if compute_on:
            compute(t, between)
        else:
            between(0)
            between(1)
        if comm_on:
            start(t, "pair")
        between(2)
        return _

    if not compute_on:
        pl.semaphore_wait(barrier, 7)
    lax.fori_loop(0, n, iteration, None)
    if comm_on:
        for i, k in drain:
            step(i, k)
        lax.fori_loop(0, n, lambda i, _: gone(i), None)
    if not compute_on:
        for i in range(n):
            rows_in(i).wait()
        loads[6].wait()


def solution(mesh, compute_on=True, comm_on=True):
    def step(x, gain, wq, wk, wv, wo):
        rows, width = x.shape
        inner = wq.shape[1]
        heads, n = inner // HEAD, rows // CH
        base, local = tables()
        f32, bf16 = jnp.float32, jnp.bfloat16
        vmem, hbm = pl.BlockSpec(memory_space=pltpu.VMEM), pl.BlockSpec(memory_space=pltpu.HBM)
        V = pltpu.VMEM
        return pl.pallas_call(
            functools.partial(kernel, compute_on, comm_on),
            out_shape=pltpu.VMEM((rows, width), bf16),
            in_specs=[hbm] * 8,
            out_specs=vmem,
            scratch_shapes=[
                V(base.shape, f32), V(local.shape, f32), V((width,), bf16), V((rows, width), bf16),
                *[V((width, inner), bf16)] * 3, V((inner, width), bf16), V((inner, width), bf16),
                V((rows, inner), bf16), V((inner, rows), bf16), V((CH, inner), bf16), V((CH, inner), bf16),
                V((heads, 2 * CH, CH), f32), V((heads, HEAD + 8, CH), f32),
                V((n, CH // 2, width), bf16), V((n, CH // 2, width), bf16), V((n, CH // 2, width), f32),
                V((n, 2, CH // 8, width), bf16), V((n, 2, CH // 8, width), bf16), V((n, 2, CH // 8, width), f32),
                V((n, 2, CH // 16, width), bf16), V((n, 2, CH // 16, width), bf16), V((n, 2, CH // 16, width), f32),
                V((n, 3, CH // 8, width // 4), bf16), V((n, 3, CH // 8, width // 4), bf16), V((n, CH // 8, width // 4), f32),
                pltpu.SemaphoreType.DMA((7 + n,)),
                pltpu.SemaphoreType.DMA((n,)),
                pltpu.SemaphoreType.DMA((n, 8)),
            ],
            compiler_params=pltpu.CompilerParams(collective_id=0, has_side_effects=True, vmem_limit_bytes=62849024),
            name="layer",
        )(x, gain, wq, wk, wv, wo, jnp.asarray(base), jnp.asarray(local))

    tokens, columns = P("dp", None), P(None, "tp")
    return jax.shard_map(
        step,
        mesh=mesh,
        in_specs=(tokens, P(None), columns, columns, columns, P("tp", None)),
        out_specs=tokens,
        check_vma=False,
    )
```

```python
import functools

import jax
import jax.numpy as jnp
import numpy as np
from jax import lax
from jax.experimental import pallas as pl
from jax.experimental.pallas import tpu as pltpu
from jax.sharding import PartitionSpec as P

HEAD = 128
THETA = 10000
LOG2E = 1.4426950408889634
HIDDEN = -2e30
CH = 256
NORM = 32
PROJ = 2
WO = 4
MESH = pl.DeviceIdType.MESH


def tables():
    half = HEAD // 2
    freq = THETA ** (-np.arange(half, dtype=np.float64) / half)
    freq = np.concatenate([freq, freq])
    sign = np.concatenate([-np.ones(half), np.ones(half)])

    def pair(place):
        angle = place[:, None] * freq
        return np.stack([np.cos(angle), np.sin(angle) * sign]).astype(np.float32)

    return pair(np.arange(8) * CH), pair(np.arange(CH))


LONG = ("pair", "first", "second", "line", "line back", "second back", "first back", "pair back")
SHORT = ("pair", "plane", "line", "line back", "plane back", "pair back")
QUICK = 2


def path(i, n):
    return SHORT if i >= n - QUICK else LONG


PLAN = [[], [], [], [], [], [0], [1], [], [], [0], [2], [1], [3, 0], [], [1, 2], [], [3, 0, 2, 4], [], [1, 3, 5], [4], [2, 0], [5, 6, 4], [3], [], [2, 5, 1, 7, 4, 3, 6, 2, 5, 1, 4, 7, 6, 0, 2, 3, 5, 4, 7, 6, 7, 2, 3, 0, 4, 5, 4, 1, 6, 0, 7, 1, 5, 6, 7, 3, 5]]


def layout(n):
    taken = [0] * n
    steps = []
    for chunks in PLAN:
        steps.append([])
        for i in chunks:
            taken[i] += 1
            steps[-1].append((i, taken[i]))
    return {(t, spot): steps[3 * t + spot] for t in range(n) for spot in range(3)}, steps[-1]


def dot(a, b, ca, cb):
    return lax.dot_general(a, b, (((ca,), (cb,)), ((), ())), preferred_element_type=jnp.float32)


def kernel(compute_on, comm_on, x_hbm, gain_hbm, wq_hbm, wk_hbm, wv_hbm, wo_hbm, base_hbm, local_hbm, y_s,
           base_ref, local_ref, gain_ref, xs, wq, wk, wv, wo, wvt, ks, vts, qs, seen_s, normed, s_s, acc_s,
           send0, recv0, keep0, send1, recv1, keep1, send2, recv2, keep2, send3, recv3, keep3,
           load_sem, send_sem, recv_sem):
    f32, bf16 = jnp.float32, jnp.bfloat16
    rows, width = xs.shape
    n = rows // CH
    heads = ks.shape[1] // HEAD
    half, quarter = CH // 2, CH // 4
    eighth, last_rows = CH // 8, CH // 16
    cols = width // 4

    me = lax.axis_index("tp")
    c, z, by, bx = lax.rem(me, 2), lax.rem(me // 2, 4), lax.rem(me // 8, 2), me // 16
    p0 = me + 1 - 2 * c
    px, py = me + 16 * (1 - 2 * bx), me + 8 * (1 - 2 * by)
    b1, b2 = (bx, by), (by, bx)
    p1, p2, p12 = (px, py), (py, px), px + py - me
    zs = [lax.rem(z + d, 4) for d in (1, 2, 3)]
    pz = [me + 2 * (to - z) for to in zs]

    barrier = pltpu.get_barrier_semaphore()
    for other in (p0, px, py, p12, *pz):
        pl.semaphore_signal(barrier, inc=1, device_id={"tp": other}, device_id_type=MESH)

    loads = [pltpu.make_async_copy(a, b, load_sem.at[i]) for i, (a, b) in enumerate(
        ((gain_hbm, gain_ref), (wv_hbm, wv), (base_hbm, base_ref), (local_hbm, local_ref), (wq_hbm, wq), (wk_hbm, wk), (wo_hbm, wo)))]

    def rows_in(i):
        at = pl.ds(pl.multiple_of(i * CH, CH), CH)
        return pltpu.make_async_copy(x_hbm.at[at], xs.at[at], load_sem.at[7 + i])

    rows_in(0).start()
    for copy in loads:
        copy.start()
    for i in range(1, n):
        rows_in(i).start()
    vts[...] = jnp.zeros(vts.shape, bf16)
    e = HEAD**-0.5 * LOG2E

    def norm(i):
        gain = gain_ref[...].reshape(1, width).astype(f32)
        for r in range(0, CH, NORM):
            wide = xs[pl.ds(pl.multiple_of(i * CH + r, NORM), NORM), :].astype(f32)
            scale = lax.rsqrt(jnp.mean(wide * wide, -1, keepdims=True) + 1e-6)
            normed[r : r + NORM, :] = (wide * scale * gain).astype(bf16)

    def compute(i, between):
        here = pl.ds(pl.multiple_of(i * CH, CH), CH)
        a = normed[...]
        cb, sb = local_ref[0], local_ref[1]
        ca, sa = base_ref[0, pl.ds(i, 1), :], base_ref[1, pl.ds(i, 1), :]
        cos, sin = ca * cb - sa * sb, sa * cb + ca * sb

        def turned(t):
            t = t.astype(bf16).astype(f32)
            return jnp.concatenate(
                [t[:, h : h + HEAD] * cos + pltpu.roll(t[:, h : h + HEAD], HEAD // 2, 1) * sin for h in range(0, t.shape[1], HEAD)], 1
            ).astype(bf16)

        for h in range(0, heads, PROJ):
            some = slice(h * HEAD, (h + PROJ) * HEAD)
            qs[:, some] = turned(dot(a, wq[:, some], 1, 0))
        for h in range(0, heads, PROJ):
            some = slice(h * HEAD, (h + PROJ) * HEAD)
            ks[here, some] = turned(dot(a, wk[:, some], 1, 0))
        vts[:, here] = dot(wvt[...], a, 1, 1).astype(bf16)

        last = i // 2
        ones = jnp.ones((8, 2 * CH), bf16)

        def scores(h, j, masked):
            at = pl.ds(pl.multiple_of(j * 2 * CH, 2 * CH), 2 * CH)
            s = dot(ks[at, h * HEAD : (h + 1) * HEAD], qs[:, h * HEAD : (h + 1) * HEAD], 1, 1) * e
            if masked:
                gap = lax.broadcasted_iota(jnp.int32, s.shape, 1) - lax.broadcasted_iota(jnp.int32, s.shape, 0)
                s = jnp.where(gap >= j * 2 * CH - i * CH, s, HIDDEN)
            s_s[h] = s
            return s.max(0, keepdims=True)

        def weigh(h, j, s, before, top):
            at = pl.ds(pl.multiple_of(j * 2 * CH, 2 * CH), 2 * CH)
            p = jnp.exp2(s - top).astype(bf16)
            values = jnp.concatenate([vts[h * HEAD : (h + 1) * HEAD, at], ones], 0)
            acc_s[h] = acc_s[h] * jnp.exp2(before - top) + dot(values, p, 1, 0)

        for h in range(heads):
            acc_s[h] = jnp.zeros(acc_s.shape[1:], f32)
        tops = tuple(scores(h, last, True) for h in range(heads))

        def trip(j, carry):
            got = []
            for h, (before, top) in enumerate(carry):
                s = s_s[h]
                new = scores(h, j, False)
                weigh(h, jnp.where(j == 0, last, j - 1), s, before, top)
                got.append((top, jnp.maximum(top, new)))
            return tuple(got)

        @pl.when(i == 0)
        def _():
            pl.semaphore_wait(barrier, 7)
            loads[6].wait()

        @pl.when(i < n - 1)
        def _():
            rows_in(i + 1).wait()

        between(0)
        tops = lax.fori_loop(0, last, trip, tuple((t, t) for t in tops))

        between(1)

        theirs = pl.ds(pl.multiple_of((1 - c) * half, half), half)
        mine = pl.ds(pl.multiple_of(c * half, half), half)
        totals = [0.0, 0.0]
        for h in range(heads):
            weigh(h, jnp.maximum(last - 1, 0), s_s[h], *tops[h])
            o = acc_s[h, :HEAD] * (1 / acc_s[h, HEAD : HEAD + 1])
            seen_s[:, h * HEAD : (h + 1) * HEAD] = o.astype(bf16).T
            if h % WO == WO - 1:
                some = slice((h + 1 - WO) * HEAD, (h + 1) * HEAD)
                totals = [t + dot(seen_s[at, some], wo[some, :], 1, 0) for t, at in zip(totals, (theirs, mine))]
        norm(jnp.minimum(i + 1, n - 1))
        send0[i] = totals[0].astype(bf16)
        keep0[i] = totals[1]

    SLOT = {"pair": 0, "first": 1, "plane": 1, "second": 2, "line": 3, "line back": 4, "second back": 5, "plane back": 5, "first back": 6, "pair back": 7}
    ROWS = {"pair": half, "first": quarter, "plane": quarter + eighth, "second": eighth, "line": 3 * eighth // 4, "line back": 3 * eighth // 4,
            "second back": eighth, "plane back": quarter + eighth, "first back": quarter, "pair back": half}

    def copy(i, move, src, dst, to):
        return pltpu.make_async_remote_copy(
            src_ref=src, dst_ref=dst, send_sem=send_sem.at[i], recv_sem=recv_sem.at[i, SLOT[move]],
            device_id={"tp": to}, device_id_type=MESH)

    def place(i, level, o):
        at = i * CH + c * half
        if level > 1:
            at += o * quarter
        if level > 2:
            at += b1[o] * eighth
        if level > 3:
            at += b2[o] * last_rows
        return pl.ds(pl.multiple_of(at, last_rows), (CH, half, quarter, eighth, last_rows)[level])

    def pieces(i, o):
        return y_s.at[place(i, 4, o), pl.ds(pl.multiple_of(z * cols, cols), cols)]

    low, high = pl.ds(0, last_rows), pl.ds(last_rows, last_rows)
    corners = ((1 - bx, by, px), (bx, 1 - by, py), (1 - bx, 1 - by, p12))

    def corner(x, y):
        return pl.multiple_of(x * quarter + y * eighth, eighth)

    def place_short(i):
        return pl.ds(pl.multiple_of(i * CH + c * half, half) + corner(bx, by), eighth)

    def copies(i, move):
        made = []

        def add(src, dst, to):
            made.append(copy(i, move, src, dst, to))

        if move == "pair":
            add(send0.at[i], recv0.at[i], p0)
        if move == "line":
            for d in range(3):
                add(send3.at[i, d], recv3.at[i, d], pz[d])
        if move == "pair back":
            add(y_s.at[place(i, 1, 0)], y_s.at[place(i, 1, 0)], p0)
        if move == "plane":
            for buf, other, (_, _, to) in zip((send1.at[i, 0], send1.at[i, 1], send2.at[i]), (recv1.at[i, 0], recv1.at[i, 1], recv2.at[i]), corners):
                add(buf, other, to)
        if move == "plane back":
            own = y_s.at[place_short(i)]
            for _, _, to in corners:
                add(own, own, to)
        if move == "line back" and path(i, n) is SHORT:
            own = y_s.at[place_short(i), pl.ds(pl.multiple_of(z * cols, cols), cols)]
            for d in range(3):
                add(own, own, pz[d])
            return made
        for o in (0, 1):
            own = y_s.at[place(i, 4, o)]
            if move == "first":
                add(send1.at[i, o], recv1.at[i, o], p1[o])
            if move == "second":
                add(send2.at[i, (low, high)[o]], recv2.at[i, (low, high)[o]], p2[o])
            if move == "line back":
                for d in range(3):
                    add(pieces(i, o), pieces(i, o), pz[d])
            if move == "second back":
                add(own, own, p2[o])
            if move == "first back":
                add(y_s.at[place(i, 3, o)], y_s.at[place(i, 3, o)], p1[o])
        return made

    def start(i, move):
        for one in copies(i, move):
            one.start()

    def arrive(i, move):
        some = y_s.at[pl.ds(0, ROWS[move])]
        copy(i, move, some, some, p0).wait_recv()

    def gone(i):
        some = y_s.at[pl.ds(0, sum(ROWS[move] for move in LONG))]
        copy(i, "pair", some, some, p0).wait_send()

    def step(i, k):
        moves = path(i, n)
        came, move = moves[k - 1], moves[k] if k < len(moves) else None
        arrive(i, came)
        def pair_sum(at, size):
            at = pl.ds(at, size)
            return keep0[i, at, :] + recv0[i, at, :].astype(f32)

        for o in (0, 1):
            there = (low, high)[o]
            if move == "first":
                keep1[i, o] = pair_sum(pl.multiple_of(o * quarter + b1[o] * eighth, eighth), eighth)
                send1[i, o] = pair_sum(pl.multiple_of(o * quarter + (1 - b1[o]) * eighth, eighth), eighth).astype(bf16)
            if move == "second":
                for flip in (False, True):
                    at = pl.ds(pl.multiple_of((1 - b2[o] if flip else b2[o]) * last_rows, last_rows), last_rows)
                    total = keep1[i, o, at, :] + recv1[i, o, at, :].astype(f32)
                    if flip:
                        send2[i, there] = total.astype(bf16)
                    else:
                        keep2[i, there] = total
        if move == "plane":
            for d, (x, y, _) in enumerate(corners):
                total = pair_sum(corner(x, y), eighth).astype(bf16)
                if d == 2:
                    send2[i] = total
                else:
                    send1[i, d] = total
            keep2[i] = pair_sum(corner(bx, by), eighth)
        if move == "line":
            for d, to in enumerate([*zs, z]):
                at = pl.ds(pl.multiple_of(to * cols, cols), cols)
                total = keep2[i, :, at] + recv2[i, :, at].astype(f32)
                if came == "plane":
                    total += recv1[i, 0, :, at].astype(f32) + recv1[i, 1, :, at].astype(f32)
                if d == 3:
                    keep3[i] = total
                else:
                    send3[i, d] = total.astype(bf16)
        if move == "line back":
            at = pl.ds(pl.multiple_of(z * cols, cols), cols)
            parts = [(slice(None), place_short(i))] if moves is SHORT else [(low, place(i, 4, 0)), (high, place(i, 4, 1))]
            for here, there in parts:
                total = keep3[i, here]
                for d in range(3):
                    total += recv3[i, d, here].astype(f32)
                y_s[there, at] = (total + xs[there, at].astype(f32)).astype(bf16)
        if move is not None:
            start(i, move)

    sites, drain = layout(n)

    def iteration(t, _):
        def between(spot):
            if comm_on:
                for when in range(n):
                    if sites[when, spot]:
                        @pl.when(t == when)
                        def _():
                            for i, k in sites[when, spot]:
                                step(i, k)

        if compute_on:
            compute(t, between)
        else:
            between(0)
            between(1)
        if comm_on:
            start(t, "pair")
        between(2)
        return _

    loads[0].wait()
    rows_in(0).wait()
    norm(0)
    loads[1].wait()
    wvt[...] = wv[...].T
    for at in (2, 3, 4, 5):
        loads[at].wait()
    if not compute_on:
        pl.semaphore_wait(barrier, 7)
    lax.fori_loop(0, n, iteration, None)
    if comm_on:
        for i, k in drain:
            step(i, k)
        lax.fori_loop(0, n, lambda i, _: gone(i), None)
    if not compute_on:
        for i in range(1, n):
            rows_in(i).wait()
        loads[6].wait()


def solution(mesh, compute_on=True, comm_on=True):
    def step(x, gain, wq, wk, wv, wo):
        rows, width = x.shape
        inner = wq.shape[1]
        heads, n = inner // HEAD, rows // CH
        base, local = tables()
        f32, bf16 = jnp.float32, jnp.bfloat16
        vmem, hbm = pl.BlockSpec(memory_space=pltpu.VMEM), pl.BlockSpec(memory_space=pltpu.HBM)
        V = pltpu.VMEM
        return pl.pallas_call(
            functools.partial(kernel, compute_on, comm_on),
            out_shape=pltpu.VMEM((rows, width), bf16),
            in_specs=[hbm] * 8,
            out_specs=vmem,
            scratch_shapes=[
                V(base.shape, f32), V(local.shape, f32), V((width,), bf16), V((rows, width), bf16),
                *[V((width, inner), bf16)] * 3, V((inner, width), bf16), V((inner, width), bf16),
                V((rows, inner), bf16), V((inner, rows), bf16), V((CH, inner), bf16), V((CH, inner), bf16),
                V((CH, width), bf16),
                V((heads, 2 * CH, CH), f32), V((heads, HEAD + 8, CH), f32),
                V((n, CH // 2, width), bf16), V((n, CH // 2, width), bf16), V((n, CH // 2, width), f32),
                V((n, 2, CH // 8, width), bf16), V((n, 2, CH // 8, width), bf16), V((n, 2, CH // 8, width), f32),
                V((n, CH // 8, width), bf16), V((n, CH // 8, width), bf16), V((n, CH // 8, width), f32),
                V((n, 3, CH // 8, width // 4), bf16), V((n, 3, CH // 8, width // 4), bf16), V((n, CH // 8, width // 4), f32),
                pltpu.SemaphoreType.DMA((7 + n,)),
                pltpu.SemaphoreType.DMA((n,)),
                pltpu.SemaphoreType.DMA((n, 8)),
            ],
            compiler_params=pltpu.CompilerParams(collective_id=0, has_side_effects=True, vmem_limit_bytes=62849024),
            name="layer",
        )(x, gain, wq, wk, wv, wo, jnp.asarray(base), jnp.asarray(local))

    tokens, columns = P("dp", None), P(None, "tp")
    return jax.shard_map(
        step,
        mesh=mesh,
        in_specs=(tokens, P(None), columns, columns, columns, P("tp", None)),
        out_specs=tokens,
        check_vma=False,
    )
```

```python
import functools

import jax
import jax.numpy as jnp
import numpy as np
from jax import lax
from jax.experimental import pallas as pl
from jax.experimental.pallas import tpu as pltpu
from jax.sharding import PartitionSpec as P

HEAD = 128
THETA = 10000
LOG2E = 1.4426950408889634
HIDDEN = -2e30
CH = 256
NORM = 32
PROJ = 2
WO = 4
MESH = pl.DeviceIdType.MESH


def tables():
    half = HEAD // 2
    freq = THETA ** (-np.arange(half, dtype=np.float64) / half)
    freq = np.concatenate([freq, freq])
    sign = np.concatenate([-np.ones(half), np.ones(half)])

    def pair(place):
        angle = place[:, None] * freq
        return np.stack([np.cos(angle), np.sin(angle) * sign]).astype(np.float32)

    return pair(np.arange(8) * CH), pair(np.arange(CH))


LONG = ("pair", "first", "second", "line", "line back", "second back", "first back", "pair back")
SHORT = ("pair", "plane", "line", "line back", "plane back", "pair back")
QUICK = 2


def path(i, n):
    return SHORT if i >= n - QUICK else LONG


PLAN = [[], [], [], [], [], [0], [1], [], [], [0], [2], [1], [3, 0], [], [1, 2], [], [3, 0, 2, 4], [], [1, 3, 5], [4], [2, 0], [5, 6, 4], [3], [], [2, 5, 1, 7, 4, 3, 6, 2, 5, 1, 4, 7, 6, 0, 2, 3, 5, 4, 7, 6, 7, 2, 3, 0, 4, 5, 4, 1, 6, 0, 7, 1, 5, 6, 7, 3, 5]]


def layout(n):
    taken = [0] * n
    steps = []
    for chunks in PLAN:
        steps.append([])
        for i in chunks:
            taken[i] += 1
            steps[-1].append((i, taken[i]))
    return {(t, spot): steps[3 * t + spot] for t in range(n) for spot in range(3)}, steps[-1]


def dot(a, b, ca, cb):
    return lax.dot_general(a, b, (((ca,), (cb,)), ((), ())), preferred_element_type=jnp.float32)


def kernel(compute_on, comm_on, x_hbm, gain_hbm, wq_hbm, wk_hbm, wv_hbm, wo_hbm, base_hbm, local_hbm, y_s,
           base_ref, local_ref, gain_ref, xs, wq, wk, wv, wo, wvt, ks, vts, qs, seen_s, normed, s_s, acc_s,
           send0, recv0, keep0, send1, recv1, keep1, send2, recv2, keep2, send3, recv3, keep3,
           load_sem, send_sem, recv_sem):
    f32, bf16 = jnp.float32, jnp.bfloat16
    rows, width = xs.shape
    n = rows // CH
    heads = ks.shape[1] // HEAD
    half, quarter = CH // 2, CH // 4
    eighth, last_rows = CH // 8, CH // 16
    cols = width // 4

    me = lax.axis_index("tp")
    c, z, by, bx = lax.rem(me, 2), lax.rem(me // 2, 4), lax.rem(me // 8, 2), me // 16
    p0 = me + 1 - 2 * c
    px, py = me + 16 * (1 - 2 * bx), me + 8 * (1 - 2 * by)
    b1, b2 = (bx, by), (by, bx)
    p1, p2, p12 = (px, py), (py, px), px + py - me
    zs = [lax.rem(z + d, 4) for d in (1, 2, 3)]
    pz = [me + 2 * (to - z) for to in zs]

    barrier = pltpu.get_barrier_semaphore()
    for other in (p0, px, py, p12, *pz):
        pl.semaphore_signal(barrier, inc=1, device_id={"tp": other}, device_id_type=MESH)

    loads = [pltpu.make_async_copy(a, b, load_sem.at[i]) for i, (a, b) in enumerate(
        ((gain_hbm, gain_ref), (wv_hbm, wv), (base_hbm, base_ref), (local_hbm, local_ref), (wq_hbm, wq), (wk_hbm, wk), (wo_hbm, wo)))]

    def rows_in(i):
        at = pl.ds(pl.multiple_of(i * CH, CH), CH)
        return pltpu.make_async_copy(x_hbm.at[at], xs.at[at], load_sem.at[7 + i])

    rows_in(0).start()
    for copy in loads[:6]:
        copy.start()
    vts[...] = jnp.zeros(vts.shape, bf16)
    e = HEAD**-0.5 * LOG2E

    def norm(i):
        gain = gain_ref[...].reshape(1, width).astype(f32)
        for r in range(0, CH, NORM):
            wide = xs[pl.ds(pl.multiple_of(i * CH + r, NORM), NORM), :].astype(f32)
            scale = lax.rsqrt(jnp.mean(wide * wide, -1, keepdims=True) + 1e-6)
            normed[r : r + NORM, :] = (wide * scale * gain).astype(bf16)

    def compute(i, between):
        here = pl.ds(pl.multiple_of(i * CH, CH), CH)
        a = normed[...]
        cb, sb = local_ref[0], local_ref[1]
        ca, sa = base_ref[0, pl.ds(i, 1), :], base_ref[1, pl.ds(i, 1), :]
        cos, sin = ca * cb - sa * sb, sa * cb + ca * sb

        def turned(t):
            t = t.astype(bf16).astype(f32)
            return jnp.concatenate(
                [t[:, h : h + HEAD] * cos + pltpu.roll(t[:, h : h + HEAD], HEAD // 2, 1) * sin for h in range(0, t.shape[1], HEAD)], 1
            ).astype(bf16)

        for h in range(0, heads, PROJ):
            some = slice(h * HEAD, (h + PROJ) * HEAD)
            qs[:, some] = turned(dot(a, wq[:, some], 1, 0))
        for h in range(0, heads, PROJ):
            some = slice(h * HEAD, (h + PROJ) * HEAD)
            ks[here, some] = turned(dot(a, wk[:, some], 1, 0))
        vts[:, here] = dot(wvt[...], a, 1, 1).astype(bf16)

        last = i // 2
        ones = jnp.ones((8, 2 * CH), bf16)

        def scores(h, j, masked):
            at = pl.ds(pl.multiple_of(j * 2 * CH, 2 * CH), 2 * CH)
            s = dot(ks[at, h * HEAD : (h + 1) * HEAD], qs[:, h * HEAD : (h + 1) * HEAD], 1, 1) * e
            if masked:
                gap = lax.broadcasted_iota(jnp.int32, s.shape, 1) - lax.broadcasted_iota(jnp.int32, s.shape, 0)
                s = jnp.where(gap >= j * 2 * CH - i * CH, s, HIDDEN)
            s_s[h] = s
            return s.max(0, keepdims=True)

        def weigh(h, j, s, before, top):
            at = pl.ds(pl.multiple_of(j * 2 * CH, 2 * CH), 2 * CH)
            p = jnp.exp2(s - top).astype(bf16)
            values = jnp.concatenate([vts[h * HEAD : (h + 1) * HEAD, at], ones], 0)
            acc_s[h] = acc_s[h] * jnp.exp2(before - top) + dot(values, p, 1, 0)

        for h in range(heads):
            acc_s[h] = jnp.zeros(acc_s.shape[1:], f32)
        tops = tuple(scores(h, last, True) for h in range(heads))

        def trip(j, carry):
            got = []
            for h, (before, top) in enumerate(carry):
                s = s_s[h]
                new = scores(h, j, False)
                weigh(h, jnp.where(j == 0, last, j - 1), s, before, top)
                got.append((top, jnp.maximum(top, new)))
            return tuple(got)

        @pl.when(i == 0)
        def _():
            pl.semaphore_wait(barrier, 7)
            loads[6].wait()

        @pl.when(i < n - 1)
        def _():
            rows_in(i + 1).wait()

        between(0)
        tops = lax.fori_loop(0, last, trip, tuple((t, t) for t in tops))

        between(1)

        theirs = pl.ds(pl.multiple_of((1 - c) * half, half), half)
        mine = pl.ds(pl.multiple_of(c * half, half), half)
        totals = [0.0, 0.0]
        for h in range(heads):
            weigh(h, jnp.maximum(last - 1, 0), s_s[h], *tops[h])
            o = acc_s[h, :HEAD] * (1 / acc_s[h, HEAD : HEAD + 1])
            seen_s[:, h * HEAD : (h + 1) * HEAD] = o.astype(bf16).T
            if h % WO == WO - 1:
                some = slice((h + 1 - WO) * HEAD, (h + 1) * HEAD)
                totals = [t + dot(seen_s[at, some], wo[some, :], 1, 0) for t, at in zip(totals, (theirs, mine))]
        norm(jnp.minimum(i + 1, n - 1))
        send0[i] = totals[0].astype(bf16)
        keep0[i] = totals[1]

    SLOT = {"pair": 0, "first": 1, "plane": 1, "second": 2, "line": 3, "line back": 4, "second back": 5, "plane back": 5, "first back": 6, "pair back": 7}
    ROWS = {"pair": half, "first": quarter, "plane": quarter + eighth, "second": eighth, "line": 3 * eighth // 4, "line back": 3 * eighth // 4,
            "second back": eighth, "plane back": quarter + eighth, "first back": quarter, "pair back": half}

    def copy(i, move, src, dst, to):
        return pltpu.make_async_remote_copy(
            src_ref=src, dst_ref=dst, send_sem=send_sem.at[i], recv_sem=recv_sem.at[i, SLOT[move]],
            device_id={"tp": to}, device_id_type=MESH)

    def place(i, level, o):
        at = i * CH + c * half
        if level > 1:
            at += o * quarter
        if level > 2:
            at += b1[o] * eighth
        if level > 3:
            at += b2[o] * last_rows
        return pl.ds(pl.multiple_of(at, last_rows), (CH, half, quarter, eighth, last_rows)[level])

    def pieces(i, o):
        return y_s.at[place(i, 4, o), pl.ds(pl.multiple_of(z * cols, cols), cols)]

    low, high = pl.ds(0, last_rows), pl.ds(last_rows, last_rows)
    corners = ((1 - bx, by, px), (bx, 1 - by, py), (1 - bx, 1 - by, p12))

    def corner(x, y):
        return pl.multiple_of(x * quarter + y * eighth, eighth)

    def place_short(i):
        return pl.ds(pl.multiple_of(i * CH + c * half, half) + corner(bx, by), eighth)

    def copies(i, move):
        made = []

        def add(src, dst, to):
            made.append(copy(i, move, src, dst, to))

        if move == "pair":
            add(send0.at[i], recv0.at[i], p0)
        if move == "line":
            for d in range(3):
                add(send3.at[i, d], recv3.at[i, d], pz[d])
        if move == "pair back":
            add(y_s.at[place(i, 1, 0)], y_s.at[place(i, 1, 0)], p0)
        if move == "plane":
            for buf, other, (_, _, to) in zip((send1.at[i, 0], send1.at[i, 1], send2.at[i]), (recv1.at[i, 0], recv1.at[i, 1], recv2.at[i]), corners):
                add(buf, other, to)
        if move == "plane back":
            own = y_s.at[place_short(i)]
            for _, _, to in corners:
                add(own, own, to)
        if move == "line back" and path(i, n) is SHORT:
            own = y_s.at[place_short(i), pl.ds(pl.multiple_of(z * cols, cols), cols)]
            for d in range(3):
                add(own, own, pz[d])
            return made
        for o in (0, 1):
            own = y_s.at[place(i, 4, o)]
            if move == "first":
                add(send1.at[i, o], recv1.at[i, o], p1[o])
            if move == "second":
                add(send2.at[i, (low, high)[o]], recv2.at[i, (low, high)[o]], p2[o])
            if move == "line back":
                for d in range(3):
                    add(pieces(i, o), pieces(i, o), pz[d])
            if move == "second back":
                add(own, own, p2[o])
            if move == "first back":
                add(y_s.at[place(i, 3, o)], y_s.at[place(i, 3, o)], p1[o])
        return made

    def start(i, move):
        for one in copies(i, move):
            one.start()

    def arrive(i, move):
        some = y_s.at[pl.ds(0, ROWS[move])]
        copy(i, move, some, some, p0).wait_recv()

    def gone(i):
        some = y_s.at[pl.ds(0, sum(ROWS[move] for move in LONG))]
        copy(i, "pair", some, some, p0).wait_send()

    def step(i, k):
        moves = path(i, n)
        came, move = moves[k - 1], moves[k] if k < len(moves) else None
        arrive(i, came)
        def pair_sum(at, size):
            at = pl.ds(at, size)
            return keep0[i, at, :] + recv0[i, at, :].astype(f32)

        for o in (0, 1):
            there = (low, high)[o]
            if move == "first":
                keep1[i, o] = pair_sum(pl.multiple_of(o * quarter + b1[o] * eighth, eighth), eighth)
                send1[i, o] = pair_sum(pl.multiple_of(o * quarter + (1 - b1[o]) * eighth, eighth), eighth).astype(bf16)
            if move == "second":
                for flip in (False, True):
                    at = pl.ds(pl.multiple_of((1 - b2[o] if flip else b2[o]) * last_rows, last_rows), last_rows)
                    total = keep1[i, o, at, :] + recv1[i, o, at, :].astype(f32)
                    if flip:
                        send2[i, there] = total.astype(bf16)
                    else:
                        keep2[i, there] = total
        if move == "plane":
            for d, (x, y, _) in enumerate(corners):
                total = pair_sum(corner(x, y), eighth).astype(bf16)
                if d == 2:
                    send2[i] = total
                else:
                    send1[i, d] = total
            keep2[i] = pair_sum(corner(bx, by), eighth)
        if move == "line":
            for d, to in enumerate([*zs, z]):
                at = pl.ds(pl.multiple_of(to * cols, cols), cols)
                total = keep2[i, :, at] + recv2[i, :, at].astype(f32)
                if came == "plane":
                    total += recv1[i, 0, :, at].astype(f32) + recv1[i, 1, :, at].astype(f32)
                if d == 3:
                    keep3[i] = total
                else:
                    send3[i, d] = total.astype(bf16)
        if move == "line back":
            at = pl.ds(pl.multiple_of(z * cols, cols), cols)
            parts = [(slice(None), place_short(i))] if moves is SHORT else [(low, place(i, 4, 0)), (high, place(i, 4, 1))]
            for here, there in parts:
                total = keep3[i, here]
                for d in range(3):
                    total += recv3[i, d, here].astype(f32)
                y_s[there, at] = (total + xs[there, at].astype(f32)).astype(bf16)
        if move is not None:
            start(i, move)

    sites, drain = layout(n)

    def iteration(t, _):
        def between(spot):
            if comm_on:
                for when in range(n):
                    if sites[when, spot]:
                        @pl.when(t == when)
                        def _():
                            for i, k in sites[when, spot]:
                                step(i, k)

        if compute_on:
            compute(t, between)
        else:
            between(0)
            between(1)
        if comm_on:
            start(t, "pair")
        between(2)
        return _

    loads[0].wait()
    rows_in(0).wait()
    norm(0)
    loads[1].wait()
    wvt[...] = wv[...].T
    for at in (2, 3, 4, 5):
        loads[at].wait()
    loads[6].start()
    for i in range(1, n):
        rows_in(i).start()
    if not compute_on:
        pl.semaphore_wait(barrier, 7)
    lax.fori_loop(0, n, iteration, None)
    if comm_on:
        for i, k in drain:
            step(i, k)
        lax.fori_loop(0, n, lambda i, _: gone(i), None)
    if not compute_on:
        for i in range(1, n):
            rows_in(i).wait()
        loads[6].wait()


def solution(mesh, compute_on=True, comm_on=True):
    def step(x, gain, wq, wk, wv, wo):
        rows, width = x.shape
        inner = wq.shape[1]
        heads, n = inner // HEAD, rows // CH
        base, local = tables()
        f32, bf16 = jnp.float32, jnp.bfloat16
        vmem, hbm = pl.BlockSpec(memory_space=pltpu.VMEM), pl.BlockSpec(memory_space=pltpu.HBM)
        V = pltpu.VMEM
        return pl.pallas_call(
            functools.partial(kernel, compute_on, comm_on),
            out_shape=pltpu.VMEM((rows, width), bf16),
            in_specs=[hbm] * 8,
            out_specs=vmem,
            scratch_shapes=[
                V(base.shape, f32), V(local.shape, f32), V((width,), bf16), V((rows, width), bf16),
                *[V((width, inner), bf16)] * 3, V((inner, width), bf16), V((inner, width), bf16),
                V((rows, inner), bf16), V((inner, rows), bf16), V((CH, inner), bf16), V((CH, inner), bf16),
                V((CH, width), bf16),
                V((heads, 2 * CH, CH), f32), V((heads, HEAD + 8, CH), f32),
                V((n, CH // 2, width), bf16), V((n, CH // 2, width), bf16), V((n, CH // 2, width), f32),
                V((n, 2, CH // 8, width), bf16), V((n, 2, CH // 8, width), bf16), V((n, 2, CH // 8, width), f32),
                V((n, CH // 8, width), bf16), V((n, CH // 8, width), bf16), V((n, CH // 8, width), f32),
                V((n, 3, CH // 8, width // 4), bf16), V((n, 3, CH // 8, width // 4), bf16), V((n, CH // 8, width // 4), f32),
                pltpu.SemaphoreType.DMA((7 + n,)),
                pltpu.SemaphoreType.DMA((n,)),
                pltpu.SemaphoreType.DMA((n, 8)),
            ],
            compiler_params=pltpu.CompilerParams(collective_id=0, has_side_effects=True, vmem_limit_bytes=62849024),
            name="layer",
        )(x, gain, wq, wk, wv, wo, jnp.asarray(base), jnp.asarray(local))

    tokens, columns = P("dp", None), P(None, "tp")
    return jax.shard_map(
        step,
        mesh=mesh,
        in_specs=(tokens, P(None), columns, columns, columns, P("tp", None)),
        out_specs=tokens,
        check_vma=False,
    )
```

```python
import functools

import jax
import jax.numpy as jnp
import numpy as np
from jax import lax
from jax.experimental import pallas as pl
from jax.experimental.pallas import tpu as pltpu
from jax.sharding import PartitionSpec as P

HEAD = 128
THETA = 10000
LOG2E = 1.4426950408889634
HIDDEN = -2e30
CH = 256
NORM = 32
PROJ = 2
WO = 4
MESH = pl.DeviceIdType.MESH


def tables():
    half = HEAD // 2
    freq = THETA ** (-np.arange(half, dtype=np.float64) / half)
    freq = np.concatenate([freq, freq])
    sign = np.concatenate([-np.ones(half), np.ones(half)])

    def pair(place):
        angle = place[:, None] * freq
        return np.stack([np.cos(angle), np.sin(angle) * sign]).astype(np.float32)

    return pair(np.arange(8) * CH), pair(np.arange(CH))


LONG = ("pair", "first", "second", "line", "line back", "second back", "first back", "pair back")
SHORT = ("pair", "plane", "line", "line back", "plane back", "pair back")
QUICK = 2


def path(i, n):
    return SHORT if i >= n - QUICK else LONG


PLAN = [[], [], [], [], [], [0], [1], [], [], [0], [2], [1], [3, 0], [], [1, 2], [], [3, 0, 2, 4], [], [1, 3, 5], [4], [2, 0], [5, 6, 4], [3], [], [2, 5, 1, 7, 4, 3, 6, 2, 5, 1, 4, 7, 6, 0, 2, 3, 5, 4, 7, 6, 7, 2, 3, 0, 4, 5, 4, 1, 6, 0, 7, 1, 5, 6, 7, 3, 5]]


def layout(n):
    taken = [0] * n
    steps = []
    for chunks in PLAN:
        steps.append([])
        for i in chunks:
            taken[i] += 1
            steps[-1].append((i, taken[i]))
    return {(t, spot): steps[3 * t + spot] for t in range(n) for spot in range(3)}, steps[-1]


def dot(a, b, ca, cb):
    return lax.dot_general(a, b, (((ca,), (cb,)), ((), ())), preferred_element_type=jnp.float32)


def kernel(compute_on, comm_on, x_hbm, gain_hbm, wq_hbm, wk_hbm, wv_hbm, wo_hbm, base_hbm, local_hbm, y_s,
           base_ref, local_ref, gain_ref, xs, wq, wk, wv, wo, wvt, ks, vts, qs, seen_s, normed, s_s, acc_s,
           send0, recv0, keep0, send1, recv1, keep1, send2, recv2, keep2, send3, recv3, keep3,
           load_sem, send_sem, recv_sem):
    f32, bf16 = jnp.float32, jnp.bfloat16
    rows, width = xs.shape
    n = rows // CH
    heads = ks.shape[1] // HEAD
    half, quarter = CH // 2, CH // 4
    eighth, last_rows = CH // 8, CH // 16
    cols = width // 4

    me = lax.axis_index("tp")
    c, z, by, bx = lax.rem(me, 2), lax.rem(me // 2, 4), lax.rem(me // 8, 2), me // 16
    p0 = me + 1 - 2 * c
    px, py = me + 16 * (1 - 2 * bx), me + 8 * (1 - 2 * by)
    b1, b2 = (bx, by), (by, bx)
    p1, p2, p12 = (px, py), (py, px), px + py - me
    zs = [lax.rem(z + d, 4) for d in (1, 2, 3)]
    pz = [me + 2 * (to - z) for to in zs]

    barrier = pltpu.get_barrier_semaphore()
    for other in (p0, px, py, p12, *pz):
        pl.semaphore_signal(barrier, inc=1, device_id={"tp": other}, device_id_type=MESH)

    loads = [pltpu.make_async_copy(a, b, load_sem.at[i]) for i, (a, b) in enumerate(
        ((gain_hbm, gain_ref), (wv_hbm, wv), (base_hbm, base_ref), (local_hbm, local_ref), (wq_hbm, wq), (wk_hbm, wk), (wo_hbm, wo)))]

    def rows_in(i):
        at = pl.ds(pl.multiple_of(i * CH, CH), CH)
        return pltpu.make_async_copy(x_hbm.at[at], xs.at[at], load_sem.at[7 + i])

    rows_in(0).start()
    for copy in loads[:6]:
        copy.start()
    vts[...] = jnp.zeros(vts.shape, bf16)
    e = HEAD**-0.5 * LOG2E

    def norm(i):
        gain = gain_ref[...].reshape(1, width).astype(f32)
        for r in range(0, CH, NORM):
            wide = xs[pl.ds(pl.multiple_of(i * CH + r, NORM), NORM), :].astype(f32)
            scale = lax.rsqrt(jnp.mean(wide * wide, -1, keepdims=True) + 1e-6)
            normed[r : r + NORM, :] = (wide * scale * gain).astype(bf16)

    def compute(i, between):
        here = pl.ds(pl.multiple_of(i * CH, CH), CH)
        a = normed[...]
        cb, sb = local_ref[0], local_ref[1]
        ca, sa = base_ref[0, pl.ds(i, 1), :], base_ref[1, pl.ds(i, 1), :]
        cos, sin = ca * cb - sa * sb, sa * cb + ca * sb

        def turned(t):
            t = t.astype(bf16).astype(f32)
            return jnp.concatenate(
                [t[:, h : h + HEAD] * cos + pltpu.roll(t[:, h : h + HEAD], HEAD // 2, 1) * sin for h in range(0, t.shape[1], HEAD)], 1
            ).astype(bf16)

        for h in range(0, heads, PROJ):
            some = slice(h * HEAD, (h + PROJ) * HEAD)
            qs[:, some] = turned(dot(a, wq[:, some], 1, 0))
        for h in range(0, heads, PROJ):
            some = slice(h * HEAD, (h + PROJ) * HEAD)
            ks[here, some] = turned(dot(a, wk[:, some], 1, 0))
        vts[:, here] = dot(wvt[...], a, 1, 1).astype(bf16)

        last = i // 2
        ones = jnp.ones((8, 2 * CH), bf16)

        def scores(h, j, masked):
            at = pl.ds(pl.multiple_of(j * 2 * CH, 2 * CH), 2 * CH)
            s = dot(ks[at, h * HEAD : (h + 1) * HEAD], qs[:, h * HEAD : (h + 1) * HEAD], 1, 1) * e
            if masked:
                gap = lax.broadcasted_iota(jnp.int32, s.shape, 1) - lax.broadcasted_iota(jnp.int32, s.shape, 0)
                s = jnp.where(gap >= j * 2 * CH - i * CH, s, HIDDEN)
            s_s[h] = s
            return s.max(0, keepdims=True)

        def weigh(h, j, s, before, top):
            at = pl.ds(pl.multiple_of(j * 2 * CH, 2 * CH), 2 * CH)
            p = jnp.exp2(s - top).astype(bf16)
            values = jnp.concatenate([vts[h * HEAD : (h + 1) * HEAD, at], ones], 0)
            acc_s[h] = acc_s[h] * jnp.exp2(before - top) + dot(values, p, 1, 0)

        for h in range(heads):
            acc_s[h] = jnp.zeros(acc_s.shape[1:], f32)
        tops = tuple(scores(h, last, True) for h in range(heads))

        def trip(j, carry):
            got = []
            for h, (before, top) in enumerate(carry):
                s = s_s[h]
                new = scores(h, j, False)
                weigh(h, jnp.where(j == 0, last, j - 1), s, before, top)
                got.append((top, jnp.maximum(top, new)))
            return tuple(got)

        @pl.when(i == 0)
        def _():
            pl.semaphore_wait(barrier, 7)
            loads[6].wait()

        @pl.when(i < n - 1)
        def _():
            rows_in(i + 1).wait()

        between(0)
        tops = lax.fori_loop(0, last, trip, tuple((t, t) for t in tops))

        between(1)

        theirs = pl.ds(pl.multiple_of((1 - c) * half, half), half)
        mine = pl.ds(pl.multiple_of(c * half, half), half)
        totals = [0.0, 0.0]
        for h in range(heads):
            weigh(h, jnp.maximum(last - 1, 0), s_s[h], *tops[h])
            o = acc_s[h, :HEAD] * (1 / acc_s[h, HEAD : HEAD + 1])
            seen_s[:, h * HEAD : (h + 1) * HEAD] = o.astype(bf16).T
            if h % WO == WO - 1:
                some = slice((h + 1 - WO) * HEAD, (h + 1) * HEAD)
                totals = [t + dot(seen_s[at, some], wo[some, :], 1, 0) for t, at in zip(totals, (theirs, mine))]
        norm(jnp.minimum(i + 1, n - 1))
        send0[i] = totals[0].astype(bf16)
        keep0[i] = totals[1]

    SLOT = {"pair": 0, "first": 1, "plane": 1, "second": 2, "line": 3, "line back": 4, "second back": 5, "plane back": 5, "first back": 6, "pair back": 7}
    ROWS = {"pair": half, "first": quarter, "plane": quarter + eighth, "second": eighth, "line": 3 * eighth // 4, "line back": 3 * eighth // 4,
            "second back": eighth, "plane back": quarter + eighth, "first back": quarter, "pair back": half}

    def copy(i, move, src, dst, to):
        return pltpu.make_async_remote_copy(
            src_ref=src, dst_ref=dst, send_sem=send_sem.at[i], recv_sem=recv_sem.at[i, SLOT[move]],
            device_id={"tp": to}, device_id_type=MESH)

    def place(i, level, o):
        at = i * CH + c * half
        if level > 1:
            at += o * quarter
        if level > 2:
            at += b1[o] * eighth
        if level > 3:
            at += b2[o] * last_rows
        return pl.ds(pl.multiple_of(at, last_rows), (CH, half, quarter, eighth, last_rows)[level])

    def pieces(i, o):
        return y_s.at[place(i, 4, o), pl.ds(pl.multiple_of(z * cols, cols), cols)]

    low, high = pl.ds(0, last_rows), pl.ds(last_rows, last_rows)
    corners = ((1 - bx, by, px), (bx, 1 - by, py), (1 - bx, 1 - by, p12))

    def corner(x, y):
        return pl.multiple_of(x * quarter + y * eighth, eighth)

    def place_short(i):
        return pl.ds(pl.multiple_of(i * CH + c * half, half) + corner(bx, by), eighth)

    def copies(i, move):
        made = []

        def add(src, dst, to):
            made.append(copy(i, move, src, dst, to))

        if move == "pair":
            add(send0.at[i], recv0.at[i], p0)
        if move == "line":
            for d in range(3):
                add(send3.at[i, d], recv3.at[i, d], pz[d])
        if move == "pair back":
            add(y_s.at[place(i, 1, 0)], y_s.at[place(i, 1, 0)], p0)
        if move == "plane":
            for buf, other, (_, _, to) in zip((send1.at[i, 0], send1.at[i, 1], send2.at[i]), (recv1.at[i, 0], recv1.at[i, 1], recv2.at[i]), corners):
                add(buf, other, to)
        if move == "plane back":
            own = y_s.at[place_short(i)]
            for _, _, to in corners:
                add(own, own, to)
        if move == "line back" and path(i, n) is SHORT:
            own = y_s.at[place_short(i), pl.ds(pl.multiple_of(z * cols, cols), cols)]
            for d in range(3):
                add(own, own, pz[d])
            return made
        for o in (0, 1):
            own = y_s.at[place(i, 4, o)]
            if move == "first":
                add(send1.at[i, o], recv1.at[i, o], p1[o])
            if move == "second":
                add(send2.at[i, (low, high)[o]], recv2.at[i, (low, high)[o]], p2[o])
            if move == "line back":
                for d in range(3):
                    add(pieces(i, o), pieces(i, o), pz[d])
            if move == "second back":
                add(own, own, p2[o])
            if move == "first back":
                add(y_s.at[place(i, 3, o)], y_s.at[place(i, 3, o)], p1[o])
        return made

    def start(i, move):
        for one in copies(i, move):
            one.start()

    def arrive(i, move):
        some = y_s.at[pl.ds(0, ROWS[move])]
        copy(i, move, some, some, p0).wait_recv()

    def gone(i):
        some = y_s.at[pl.ds(0, sum(ROWS[move] for move in LONG))]
        copy(i, "pair", some, some, p0).wait_send()

    def step(i, k):
        moves = path(i, n)
        came, move = moves[k - 1], moves[k] if k < len(moves) else None
        arrive(i, came)
        def pair_sum(at, size):
            at = pl.ds(at, size)
            return keep0[i, at, :] + recv0[i, at, :].astype(f32)

        for o in (0, 1):
            there = (low, high)[o]
            if move == "first":
                keep1[i, o] = pair_sum(pl.multiple_of(o * quarter + b1[o] * eighth, eighth), eighth)
                send1[i, o] = pair_sum(pl.multiple_of(o * quarter + (1 - b1[o]) * eighth, eighth), eighth).astype(bf16)
            if move == "second":
                for flip in (False, True):
                    at = pl.ds(pl.multiple_of((1 - b2[o] if flip else b2[o]) * last_rows, last_rows), last_rows)
                    total = keep1[i, o, at, :] + recv1[i, o, at, :].astype(f32)
                    if flip:
                        send2[i, there] = total.astype(bf16)
                    else:
                        keep2[i, there] = total
        if move == "plane":
            for d, (x, y, _) in enumerate(corners):
                total = pair_sum(corner(x, y), eighth).astype(bf16)
                if d == 2:
                    send2[i] = total
                else:
                    send1[i, d] = total
            keep2[i] = pair_sum(corner(bx, by), eighth)
        if move == "line":
            for d, to in enumerate([*zs, z]):
                at = pl.ds(pl.multiple_of(to * cols, cols), cols)
                total = keep2[i, :, at] + recv2[i, :, at].astype(f32)
                if came == "plane":
                    total += recv1[i, 0, :, at].astype(f32) + recv1[i, 1, :, at].astype(f32)
                if d == 3:
                    keep3[i] = total
                else:
                    send3[i, d] = total.astype(bf16)
        if move == "line back":
            at = pl.ds(pl.multiple_of(z * cols, cols), cols)
            parts = [(slice(None), place_short(i))] if moves is SHORT else [(low, place(i, 4, 0)), (high, place(i, 4, 1))]
            for here, there in parts:
                total = keep3[i, here]
                for d in range(3):
                    total += recv3[i, d, here].astype(f32)
                y_s[there, at] = (total + xs[there, at].astype(f32)).astype(bf16)
        if move is not None:
            start(i, move)

    sites, drain = layout(n)

    def iteration(t, _):
        def between(spot):
            if comm_on:
                for when in range(n):
                    if sites[when, spot]:
                        @pl.when(t == when)
                        def _():
                            for i, k in sites[when, spot]:
                                step(i, k)

        if compute_on:
            compute(t, between)
        else:
            between(0)
            between(1)
        if comm_on:
            start(t, "pair")
        between(2)
        return _

    loads[0].wait()
    rows_in(0).wait()
    norm(0)
    loads[1].wait()
    wvt[...] = wv[...].T
    for at in (2, 3, 4, 5):
        loads[at].wait()
    loads[6].start()
    for i in range(1, n):
        rows_in(i).start()
    if not compute_on:
        pl.semaphore_wait(barrier, 7)
    lax.fori_loop(0, n, iteration, None)
    if comm_on:
        for i, k in drain[:-1]:
            step(i, k)
        final = drain[-1][0]
        for i in range(n):
            if i != final:
                gone(i)
        step(*drain[-1])
        gone(final)
    if not compute_on:
        for i in range(1, n):
            rows_in(i).wait()
        loads[6].wait()


def solution(mesh, compute_on=True, comm_on=True):
    def step(x, gain, wq, wk, wv, wo):
        rows, width = x.shape
        inner = wq.shape[1]
        heads, n = inner // HEAD, rows // CH
        base, local = tables()
        f32, bf16 = jnp.float32, jnp.bfloat16
        vmem, hbm = pl.BlockSpec(memory_space=pltpu.VMEM), pl.BlockSpec(memory_space=pltpu.HBM)
        V = pltpu.VMEM
        return pl.pallas_call(
            functools.partial(kernel, compute_on, comm_on),
            out_shape=pltpu.VMEM((rows, width), bf16),
            in_specs=[hbm] * 8,
            out_specs=vmem,
            scratch_shapes=[
                V(base.shape, f32), V(local.shape, f32), V((width,), bf16), V((rows, width), bf16),
                *[V((width, inner), bf16)] * 3, V((inner, width), bf16), V((inner, width), bf16),
                V((rows, inner), bf16), V((inner, rows), bf16), V((CH, inner), bf16), V((CH, inner), bf16),
                V((CH, width), bf16),
                V((heads, 2 * CH, CH), f32), V((heads, HEAD + 8, CH), f32),
                V((n, CH // 2, width), bf16), V((n, CH // 2, width), bf16), V((n, CH // 2, width), f32),
                V((n, 2, CH // 8, width), bf16), V((n, 2, CH // 8, width), bf16), V((n, 2, CH // 8, width), f32),
                V((n, CH // 8, width), bf16), V((n, CH // 8, width), bf16), V((n, CH // 8, width), f32),
                V((n, 3, CH // 8, width // 4), bf16), V((n, 3, CH // 8, width // 4), bf16), V((n, CH // 8, width // 4), f32),
                pltpu.SemaphoreType.DMA((7 + n,)),
                pltpu.SemaphoreType.DMA((n,)),
                pltpu.SemaphoreType.DMA((n, 8)),
            ],
            compiler_params=pltpu.CompilerParams(collective_id=0, has_side_effects=True, vmem_limit_bytes=62849024),
            name="layer",
        )(x, gain, wq, wk, wv, wo, jnp.asarray(base), jnp.asarray(local))

    tokens, columns = P("dp", None), P(None, "tp")
    return jax.shard_map(
        step,
        mesh=mesh,
        in_specs=(tokens, P(None), columns, columns, columns, P("tp", None)),
        out_specs=tokens,
        check_vma=False,
    )
```
